32 devices in a mesh: lat: 8 (over z, x), lon: 4 (over y, core).
Axes of the slice: x: 2, y: 2, z: 4, core: 2. Of those that a mesh axis runs over, the one named last changes fastest.
Arguments:
- fields: float32 [8, 8, 128, 512], P(None, None, 'lat', 'lon'), may hold values from -6 to 6
- ocean_mask: int32 [128, 4], replicated, may hold values from 0 to 1, as said below
- scale_table: float32 [16], replicated, may hold values from 0.5 to 4
- offset_table: float32 [16], replicated, may hold values from -4 to 4
- scale_index: int32 [8], replicated, may hold values from 0 to 15
- offset_index: int32 [8], replicated, may hold values from 0 to 15
Outputs:
- history: float32 [8, 8, 128, 512], P(None, 'lat', 'lon')
- record_range: float32 [2, 8, 8], P(None, None, 'lat')
The draws below stay inside these ranges and needn't reach their ends.
Inputs may be any that keep to these rules, and one draw needn't show every extreme that they name: `ocean_mask`: each device's block of 16 rows and 128 longitudes holds at least half of 12 (rounded down, and never fewer than one) and at most 12 ocean strips; some block holds exactly 12.
All inputs are finite; a program needn't handle non-finite values.
Results may differ from the reference program's by a relative error of at most 0.00007.
Values sent between devices are 32-bit elements; how exact they have to be, the bound alone decides.
A program may use at most 64 MiB of HBM per device.

```python
import math
import jax
import jax.numpy as jnp

FIELDS = 8
TABLE = 16
LAT_DEV = 16
LON_DEV = 128
STRIP = 128
LEVELS = 8
NLAT = 128
NLON = 512
NSTRIP = 4
MAX_LIVE = 12


def draw_ocean_mask(key, part):
    strips_row = LON_DEV // STRIP
    per_block = LAT_DEV * strips_row
    blocks_lat = NLAT // LAT_DEV
    blocks_lon = NSTRIP // strips_row
    total_blocks = blocks_lat * blocks_lon
    count_key = jax.random.fold_in(key, 11)
    full_key = jax.random.fold_in(key, 12)
    score_key = jax.random.fold_in(key, 13)
    fewest = max(1, MAX_LIVE // 2)
    counts = jax.random.randint(count_key, (total_blocks,), fewest, MAX_LIVE + 1)
    full_block = jax.random.randint(full_key, (), 0, total_blocks)
    counts = jnp.where(jnp.arange(total_blocks) == full_block, MAX_LIVE, counts)
    scores = jax.random.randint(score_key, (total_blocks, per_block), 0, 1 << 20) * per_block
    scores = scores + jnp.arange(per_block)[None, :]
    ranks = jnp.argsort(jnp.argsort(scores, axis=1), axis=1)
    ocean = (ranks < counts[:, None]).astype(jnp.int32)
    ocean = ocean.reshape(blocks_lat, blocks_lon, LAT_DEV, strips_row).transpose(0, 2, 1, 3)
    return ocean.reshape(NLAT, NSTRIP)


def with_ends(entries, own_key, smallest, top_value):
    dims = entries.shape
    place = [jax.random.randint(jax.random.fold_in(own_key, axis), (), 0, dims[axis]) for axis in range(len(dims))]
    entries = entries.at[tuple(place)].set(smallest)
    longest = dims.index(max(dims))
    place[longest] = (place[longest] + 1) % dims[longest]
    return entries.at[tuple(place)].set(top_value)


def levels(own_key, extent, split, low, largest):
    loudness, own = 1.0, jax.random.fold_in(own_key, 6)
    for dim, blocks in split:
        heights = jnp.exp(jax.random.uniform(jax.random.fold_in(own, dim), (blocks,), jnp.float32, low / len(split), largest / len(split)))
        loudness = loudness * jnp.repeat(heights, extent[dim] // blocks).reshape([-1 if axis == dim else 1 for axis in range(len(extent))])
    return loudness


def bell_draw(own_key, dims, scale, limit, split=(), held_as=jnp.bfloat16):
    drawn = jax.random.normal(own_key, dims, jnp.float32) * scale
    if len(split) > 0:
        drawn = levels(own_key, dims, split, -0.22, 0.18) * drawn
    return jnp.clip(drawn, min=-limit, max=limit).astype(held_as)


def setup_inputs(seed: int = 0) -> dict:
    splits = jax.random.split(jax.random.key(seed), 7)
    return {
        "fields": bell_draw(splits[0], (FIELDS, LEVELS, NLAT, NLON), 1.0, 6.0, ((2, 8), (3, 4)), jnp.float32),
        "ocean_mask": draw_ocean_mask(jax.random.fold_in(splits[6], 71), 0),
        "scale_table": jnp.clip(jnp.exp(jax.random.uniform(splits[2], (TABLE,), jnp.float32, math.log(0.5), math.log(4.0))), 0.5, 4.0),
        "offset_table": bell_draw(splits[3], (TABLE,), 1.0, 4.0, (), jnp.float32),
        "scale_index": with_ends(jax.random.randint(splits[4], (FIELDS,), 0, TABLE), jax.random.fold_in(splits[4], 1), 0, TABLE - 1).astype(jnp.int32),
        "offset_index": with_ends(jax.random.randint(splits[5], (FIELDS,), 0, TABLE), jax.random.fold_in(splits[5], 1), 0, TABLE - 1).astype(jnp.int32),
    }


def reference(fields, ocean_mask, scale_table, offset_table, scale_index, offset_index):
    scales = scale_table[scale_index].astype(jnp.float32)
    offsets = offset_table[offset_index].astype(jnp.float32)
    ocean_cells = jnp.repeat(ocean_mask, STRIP, axis=1) > 0
    packed = (fields - offsets[:, None, None, None]) * scales[:, None, None, None]
    history = jnp.where(ocean_cells[None, None], packed, jnp.zeros_like(packed))
    highest = jnp.max(jnp.where(ocean_cells[None, None], packed, -jnp.inf), axis=(2, 3))
    lowest = jnp.min(jnp.where(ocean_cells[None, None], packed, jnp.inf), axis=(2, 3))
    return history, jnp.stack([highest, lowest])
```

```python
import functools

import jax
import jax.numpy as jnp
from jax import lax
from jax.experimental import pallas as pl
from jax.experimental.pallas import tpu as pltpu
from jax.sharding import PartitionSpec as P

STRIP = 128
MAX_LIVE = 12
MESH = pl.DeviceIdType.MESH


def kernel(
    dims, mask, scale_table, offset_table, scale_index, offset_index, x_hbm,
    out, rng,
    xv, send, recv, stage, part, stats, in_sem, send_sem, recv_sem, stat_send, stat_recv,
):
    fields, levels, rows, lat_count, lon_count = dims
    slab = lat_count // lon_count
    slots = send.shape[1]
    devices = lat_count * lon_count
    lat_pos = lax.axis_index("lat")
    lon_pos = lax.axis_index("lon")
    me = lat_pos * lon_count + lon_pos

    load = pltpu.make_async_copy(x_hbm, xv, in_sem)
    load.start()

    def peer(step):
        other = lax.rem(me + step, devices)
        return other // lon_count, lax.rem(other, lon_count)

    barrier = pltpu.get_barrier_semaphore()

    def greet(step, carry):
        pl.semaphore_signal(barrier, inc=1, device_id=peer(step), device_id_type=MESH)
        return carry

    lax.fori_loop(1, devices, greet, 0)

    seen = []
    total = jnp.int32(0)
    for r in range(rows):
        total = total + mask[lon_pos, lat_pos * rows + r]
        seen.append(total)
    picks = []
    for k in range(slots):
        slot = jnp.minimum(k, total - 1)
        pick = jnp.int32(0)
        for r in range(rows - 1):
            pick = pick + (seen[r] <= slot).astype(jnp.int32)
        picks.append(pick)

    which = lax.broadcasted_iota(jnp.int32, (fields, STRIP), 0)
    scales = jnp.zeros((fields, STRIP), jnp.float32)
    offsets = jnp.zeros((fields, STRIP), jnp.float32)
    for f in range(fields):
        scales = jnp.where(which == f, scale_table[scale_index[f]], scales)
        offsets = jnp.where(which == f, offset_table[offset_index[f]], offsets)

    load.wait()

    def pack(level, carry):
        high = None
        for k in range(slots):
            strip = xv[pl.ds(level * rows + picks[k], fields, stride=levels * rows), :]
            packed = (strip - offsets) * scales
            send[level, k] = packed
            high = packed if high is None else jnp.maximum(high, packed)
            low = -packed if k == 0 else jnp.maximum(low, -packed)
        part[pl.ds(pl.multiple_of(level * fields, fields), fields), :] = high
        part[pl.ds(pl.multiple_of((levels + level) * fields, fields), fields), :] = low
        return carry

    lax.fori_loop(0, levels, pack, 0)

    pl.semaphore_wait(barrier, devices - 1)

    slab_pos = lat_pos // slab
    here = lax.rem(lat_pos, slab) * lon_count + lon_pos

    def remote(level):
        return pltpu.make_async_remote_copy(
            src_ref=send.at[level],
            dst_ref=recv.at[here],
            send_sem=send_sem.at[level],
            recv_sem=recv_sem.at[here],
            device_id=(level, slab_pos),
            device_id_type=MESH,
        )

    def local(level):
        return pltpu.make_async_copy(send.at[level], recv.at[here], recv_sem.at[here])

    def is_self(level):
        return jnp.logical_and(level == lat_pos, slab_pos == lon_pos)

    def post(step, carry):
        level = lax.rem(lat_pos + lat_count // 2 + step, lat_count)

        @pl.when(is_self(level))
        def _():
            local(level).start()

        @pl.when(jnp.logical_not(is_self(level)))
        def _():
            remote(level).start()

        return carry

    lax.fori_loop(0, lat_count, post, 0)

    stat_rows = stats.shape[1]
    for j in range(stat_rows):
        tile = part[j * STRIP:(j + 1) * STRIP, :].T
        stats[me, j] = jnp.max(tile, axis=0, keepdims=True)

    def stat_copy(step):
        return pltpu.make_async_remote_copy(
            src_ref=stats.at[me],
            dst_ref=stats.at[me],
            send_sem=stat_send,
            recv_sem=stat_recv,
            device_id=peer(step),
            device_id_type=MESH,
        )

    def tell(step, carry):
        stat_copy(step).start()
        return carry

    lax.fori_loop(1, devices, tell, 0)

    per_field = (slab * rows) * lon_count

    for b in range(lon_count):
        for i in range(slab):
            source = i * lon_count + b
            pltpu.make_async_copy(recv.at[source], recv.at[source], recv_sem.at[source]).wait()
            stage[source] = recv[source]
            rank = jnp.int32(0)
            for r in range(rows):
                live = mask[b, (lon_pos * slab + i) * rows + r]
                strip = stage[source, jnp.minimum(rank, slots - 1)]
                strip = jnp.where(live > 0, strip, 0.0)
                row = i * rows + r
                start = (row // 8 * lon_count + b) * 8 + row % 8
                out[pl.ds(start, fields, stride=per_field), :] = strip
                rank = rank + live

    others = stats.at[pl.ds(0, devices - 1)]
    pltpu.make_async_copy(others, others, stat_recv).wait()
    for end in range(2):
        first = (end * levels + lat_pos) * fields
        best = jnp.max(stats[:, first // STRIP], axis=0)
        best = jnp.broadcast_to(best, (8, STRIP))
        own = pltpu.roll(best, lax.rem(STRIP - lax.rem(first, STRIP), STRIP), 1)
        own = own[:1, :fields]
        rng[end] = own if end == 0 else -own

    def drain(step, carry):
        level = lax.rem(lat_pos + step, lat_count)

        @pl.when(jnp.logical_not(is_self(level)))
        def _():
            remote(level).wait_send()

        return carry

    lax.fori_loop(0, lat_count, drain, 0)
    pltpu.make_async_copy(others, others, stat_send).wait()


def per_device(fields, ocean_mask, scale_table, offset_table, scale_index, offset_index):
    nfield, levels, rows, cells = fields.shape
    lat_count = lax.axis_size("lat")
    lon_count = lax.axis_size("lon")
    slab = lat_count // lon_count
    devices = lat_count * lon_count
    slots = min(MAX_LIVE, rows)
    sources = slab * lon_count
    out_rows = nfield * slab * rows * lon_count
    smem = pl.BlockSpec(memory_space=pltpu.SMEM)
    vmem = pl.BlockSpec(memory_space=pltpu.VMEM)
    history, record_range = pl.pallas_call(
        functools.partial(kernel, (nfield, levels, rows, lat_count, lon_count)),
        out_shape=(
            jax.ShapeDtypeStruct((out_rows, STRIP), jnp.float32),
            jax.ShapeDtypeStruct((2, 1, nfield), jnp.float32),
        ),
        in_specs=[smem] * 5 + [pl.BlockSpec(memory_space=pl.ANY)],
        out_specs=(vmem, vmem),
        scratch_shapes=[
            pltpu.VMEM((nfield * levels * rows, STRIP), jnp.float32),
            pltpu.VMEM((levels, slots, nfield, STRIP), jnp.float32),
            pltpu.VMEM((sources, slots, nfield, STRIP), jnp.float32),
            pltpu.VMEM((sources, slots, nfield, STRIP), jnp.float32),
            pltpu.VMEM((2 * levels * nfield, STRIP), jnp.float32),
            pltpu.VMEM((devices, 2 * levels * nfield // STRIP, 1, STRIP), jnp.float32),
            pltpu.SemaphoreType.DMA,
            pltpu.SemaphoreType.DMA((levels,)),
            pltpu.SemaphoreType.DMA((sources,)),
            pltpu.SemaphoreType.DMA,
            pltpu.SemaphoreType.DMA,
        ],
        compiler_params=pltpu.CompilerParams(collective_id=0, has_side_effects=True),
    )(
        ocean_mask.T, scale_table, offset_table, scale_index, offset_index,
        fields.reshape(nfield * levels * rows, cells),
    )
    history = history.reshape(nfield, slab * rows // 8, lon_count, 8, STRIP)
    history = history.transpose(0, 1, 3, 2, 4)
    return history.reshape(nfield, 1, slab * rows, lon_count * STRIP), record_range.reshape(2, nfield, 1)


def solution(mesh):
    return jax.shard_map(
        per_device,
        mesh=mesh,
        in_specs=(P(None, None, "lat", "lon"), P(), P(), P(), P(), P()),
        out_specs=(P(None, "lat", "lon", None), P(None, None, "lat")),
        check_vma=False,
    )
```

```python
import functools

import jax
import jax.numpy as jnp
from jax import lax
from jax.experimental import pallas as pl
from jax.experimental.pallas import tpu as pltpu
from jax.sharding import PartitionSpec as P

STRIP = 128
MAX_LIVE = 12
MESH = pl.DeviceIdType.MESH


def kernel(
    dims, mask_hbm, scale_table_hbm, offset_table_hbm, scale_index_hbm, offset_index_hbm, x_hbm,
    out, rng,
    mask, scale_table, offset_table, scale_index, offset_index,
    xv, send, recv, stage, part, first_stats, last_stats,
    in_sem, send_sem, recv_sem, stat_send, stat_recv, last_send, last_recv, from_below, from_above,
):
    fields, levels, rows, lat_count, lon_count = dims
    slab = lat_count // lon_count
    planes = lat_count // slab
    plane_size = slab * lon_count
    slots = send.shape[1]
    lat_pos = lax.axis_index("lat")
    lon_pos = lax.axis_index("lon")
    plane = lat_pos // slab
    here = lax.rem(lat_pos, slab) * lon_count + lon_pos

    barrier = pltpu.get_barrier_semaphore()

    def greet(step, carry):
        other = lax.rem(here + step, plane_size)
        target = (plane * slab + other // lon_count, lax.rem(other, lon_count))
        pl.semaphore_signal(barrier, inc=1, device_id=target, device_id_type=MESH)
        return carry

    lax.fori_loop(1, plane_size, greet, 0)
    has_above = plane < planes - 1
    has_below = plane > 0

    def call_above(sem):
        @pl.when(has_above)
        def _():
            pl.semaphore_signal(sem, inc=1, device_id=(lat_pos + slab, lon_pos), device_id_type=MESH)

    def call_below(sem):
        @pl.when(has_below)
        def _():
            pl.semaphore_signal(sem, inc=1, device_id=(lat_pos - slab, lon_pos), device_id_type=MESH)

    call_above(barrier)
    call_below(barrier)

    load = pltpu.make_async_copy(x_hbm, xv, in_sem.at[0])
    smalls = [
        pltpu.make_async_copy(src, dst, in_sem.at[n + 1])
        for n, (src, dst) in enumerate([
            (mask_hbm, mask), (scale_table_hbm, scale_table), (offset_table_hbm, offset_table),
            (scale_index_hbm, scale_index), (offset_index_hbm, offset_index),
        ])
    ]
    for copy in smalls:
        copy.start()
    load.start()
    for copy in smalls:
        copy.wait()

    seen = []
    total = jnp.int32(0)
    for r in range(rows):
        total = total + mask[lon_pos, lat_pos * rows + r]
        seen.append(total)
    picks = []
    for k in range(slots):
        slot = jnp.minimum(k, total - 1)
        pick = jnp.int32(0)
        for r in range(rows - 1):
            pick = pick + (seen[r] <= slot).astype(jnp.int32)
        picks.append(pick)

    which = lax.broadcasted_iota(jnp.int32, (fields, STRIP), 0)
    scales = jnp.zeros((fields, STRIP), jnp.float32)
    offsets = jnp.zeros((fields, STRIP), jnp.float32)
    for f in range(fields):
        scales = jnp.where(which == f, scale_table[scale_index[f]], scales)
        offsets = jnp.where(which == f, offset_table[offset_index[f]], offsets)

    load.wait()

    def pack(level, carry):
        high = None
        for k in range(slots):
            strip = xv[pl.ds(level * rows + picks[k], fields, stride=levels * rows), :]
            packed = (strip - offsets) * scales
            send[level, k] = packed
            high = packed if k == 0 else jnp.maximum(high, packed)
            low = -packed if k == 0 else jnp.maximum(low, -packed)
        part[pl.ds(pl.multiple_of(level * fields, fields), fields), :] = high
        part[pl.ds(pl.multiple_of((levels + level) * fields, fields), fields), :] = low
        return carry

    lax.fori_loop(0, levels, pack, 0)

    neighbours = has_above.astype(jnp.int32) + has_below.astype(jnp.int32)
    pl.semaphore_wait(barrier, plane_size - 1 + neighbours)
    call_above(from_below)
    call_below(from_above)

    for j in range(first_stats.shape[1]):
        tile = part[j * STRIP:(j + 1) * STRIP, :].T
        first_stats[plane, j] = jnp.max(tile, axis=0, keepdims=True)

    def remote(level):
        return pltpu.make_async_remote_copy(
            src_ref=send.at[level],
            dst_ref=recv.at[here],
            send_sem=send_sem.at[level],
            recv_sem=recv_sem.at[here],
            device_id=(level, plane),
            device_id_type=MESH,
        )

    def tell(target):
        return pltpu.make_async_remote_copy(
            src_ref=first_stats.at[plane],
            dst_ref=first_stats.at[plane],
            send_sem=stat_send.at[target],
            recv_sem=stat_recv.at[plane],
            device_id=(target * slab + lax.rem(lat_pos, slab), lon_pos),
            device_id_type=MESH,
        )

    def is_self(level):
        return jnp.logical_and(level == lat_pos, plane == lon_pos)

    for i in range(slab):
        level = plane * slab + i

        @pl.when(is_self(level))
        def _():
            pltpu.make_async_copy(send.at[level], recv.at[here], recv_sem.at[here]).start()

        @pl.when(jnp.logical_not(is_self(level)))
        def _():
            remote(level).start()

    def pass_from_below():
        pl.semaphore_wait(from_below, 1)
        call_above(from_below)

    def pass_from_above():
        pl.semaphore_wait(from_above, 1)
        call_below(from_above)

    def post_plane(target):
        for i in range(slab):
            remote(target * slab + i).start()

    def loop(low, high, body):
        def step(n, carry):
            body(n)
            return carry

        lax.fori_loop(low, high, step, 0)

    lower = plane < planes // 2

    @pl.when(lower)
    def _():
        loop(0, plane, lambda n: pass_from_below())
        loop(0, plane, lambda n: tell(n).start())

        def up(n):
            pass_from_above()
            tell(n).start()
            post_plane(n)

        loop(plane + 1, planes, up)
        loop(0, plane, post_plane)

    @pl.when(jnp.logical_not(lower))
    def _():
        loop(plane + 1, planes, lambda n: pass_from_above())
        loop(0, plane, lambda n: pass_from_below())
        loop(0, plane, lambda n: tell(n).start())
        loop(plane + 1, planes, lambda n: tell(n).start())
        loop(0, plane, post_plane)
        loop(plane + 1, planes, post_plane)

    def others(n, body):
        @pl.when(n != plane)
        def _():
            body(n)

    loop(0, planes, lambda n: others(n, lambda m: pltpu.make_async_copy(
        first_stats.at[m], first_stats.at[m], stat_recv.at[m]).wait()))
    last_stats[here] = jnp.max(first_stats[...], axis=0)

    def share(step):
        other = lax.rem(here + step, plane_size)
        return pltpu.make_async_remote_copy(
            src_ref=last_stats.at[here],
            dst_ref=last_stats.at[here],
            send_sem=last_send.at[step],
            recv_sem=last_recv.at[step],
            device_id=(plane * slab + other // lon_count, lax.rem(other, lon_count)),
            device_id_type=MESH,
        )

    loop(1, plane_size, lambda n: share(n).start())

    per_field = (slab * rows) * lon_count

    for b in range(lon_count):
        for i in range(slab):
            source = i * lon_count + b
            pltpu.make_async_copy(recv.at[source], recv.at[source], recv_sem.at[source]).wait()
            stage[source] = recv[source]
            rank = jnp.int32(0)
            for r in range(rows):
                live = mask[b, (lon_pos * slab + i) * rows + r]
                strip = stage[source, jnp.minimum(rank, slots - 1)]
                strip = jnp.where(live > 0, strip, 0.0)
                line = i * rows + r
                start = (line // 8 * lon_count + b) * 8 + line % 8
                out[pl.ds(start, fields, stride=per_field), :] = strip
                rank = rank + live

    loop(1, plane_size, lambda n: share(n).wait())
    for end in range(2):
        first = (end * levels + lat_pos) * fields
        best = jnp.max(last_stats[:, first // STRIP], axis=0)
        best = jnp.broadcast_to(best, (8, STRIP))
        own = pltpu.roll(best, lax.rem(STRIP - lax.rem(first, STRIP), STRIP), 1)
        own = own[:1, :fields]
        rng[end] = own if end == 0 else -own

    def drain(level, carry):
        @pl.when(jnp.logical_not(is_self(level)))
        def _():
            remote(level).wait_send()

        return carry

    lax.fori_loop(0, lat_count, drain, 0)
    loop(0, planes, lambda n: others(n, lambda m: tell(m).wait_send()))


def per_device(fields, ocean_mask, scale_table, offset_table, scale_index, offset_index):
    nfield, levels, rows, cells = fields.shape
    lat_count = lax.axis_size("lat")
    lon_count = lax.axis_size("lon")
    slab = lat_count // lon_count
    slots = min(MAX_LIVE, rows)
    sources = slab * lon_count
    out_rows = nfield * slab * rows * lon_count
    hbm = pl.BlockSpec(memory_space=pltpu.HBM)
    stat_rows = 2 * levels * nfield // STRIP
    vmem = pl.BlockSpec(memory_space=pltpu.VMEM)
    history, record_range = pl.pallas_call(
        functools.partial(kernel, (nfield, levels, rows, lat_count, lon_count)),
        out_shape=(
            jax.ShapeDtypeStruct((out_rows, STRIP), jnp.float32),
            jax.ShapeDtypeStruct((2, 1, nfield), jnp.float32),
        ),
        in_specs=[hbm] * 6,
        out_specs=(vmem, vmem),
        scratch_shapes=[
            pltpu.SMEM((lon_count, lat_count * rows), jnp.int32),
            pltpu.SMEM(scale_table.shape, jnp.float32),
            pltpu.SMEM(offset_table.shape, jnp.float32),
            pltpu.SMEM(scale_index.shape, jnp.int32),
            pltpu.SMEM(offset_index.shape, jnp.int32),
            pltpu.VMEM((nfield * levels * rows, STRIP), jnp.float32),
            pltpu.VMEM((levels, slots, nfield, STRIP), jnp.float32),
            pltpu.VMEM((sources, slots, nfield, STRIP), jnp.float32),
            pltpu.VMEM((sources, slots, nfield, STRIP), jnp.float32),
            pltpu.VMEM((2 * levels * nfield, STRIP), jnp.float32),
            pltpu.VMEM((lat_count // slab, stat_rows, 1, STRIP), jnp.float32),
            pltpu.VMEM((sources, stat_rows, 1, STRIP), jnp.float32),
            pltpu.SemaphoreType.DMA((6,)),
            pltpu.SemaphoreType.DMA((levels,)),
            pltpu.SemaphoreType.DMA((sources,)),
            pltpu.SemaphoreType.DMA((lat_count // slab,)),
            pltpu.SemaphoreType.DMA((lat_count // slab,)),
            pltpu.SemaphoreType.DMA((sources,)),
            pltpu.SemaphoreType.DMA((sources,)),
            pltpu.SemaphoreType.REGULAR,
            pltpu.SemaphoreType.REGULAR,
        ],
        compiler_params=pltpu.CompilerParams(
            collective_id=0, has_side_effects=True
        ),
    )(
        ocean_mask.T, scale_table, offset_table, scale_index, offset_index,
        fields.reshape(nfield * levels * rows, cells),
    )
    history = history.reshape(nfield, slab * rows // 8, lon_count, 8, STRIP)
    history = history.transpose(0, 1, 3, 2, 4)
    return history.reshape(nfield, 1, slab * rows, lon_count * STRIP), record_range.reshape(2, nfield, 1)


def solution(mesh):
    return jax.shard_map(
        per_device,
        mesh=mesh,
        in_specs=(P(None, None, "lat", "lon"), P(), P(), P(), P(), P()),
        out_specs=(P(None, "lat", "lon", None), P(None, None, "lat")),
        check_vma=False,
    )
```
